512 devices in a mesh: blk: 64 (over y, x, z_lo), ga: 8 (over z_hi, core).
Axes of the slice: x: 4, y: 8, z: 8 (z_hi: 4, z_lo: 2; z = z_hi * 2 + z_lo), core: 2. Of those that a mesh axis runs over, the one named last changes fastest.
Arguments:
- pair_elements: bfloat16 [4096, 65536], P('ga', 'blk'), may hold values from -6 to 6
- screening: bfloat16 [4096, 4096], P('ga', 'blk'), may hold values from -0.09375 to 0.09375
- energies: float32 [1024], replicated, may hold values from 0.5 to 3
- frequencies: float32 [8], replicated, may hold values from 0.3 to 3
- qp_index: int32 [32], replicated, may hold values from 0 to 1023
- occupied: int32 [1024], replicated, may hold values 0 or 1
Outputs:
- self_energy: float32 [2, 8, 32, 32], replicated
The draws below stay inside these ranges and needn't reach their ends.
All inputs are finite; a program needn't handle non-finite values.
Results may differ from the reference program's by a relative error of at most 0.0003.
Values may be sent and summed in bfloat16 or wider, within the bound.
A program may use at most 64 MiB of HBM per device.

```python
import math
import jax
import jax.numpy as jnp
from jax import lax

STATES = 32
BAND_DEV = 16
NG = 4096
NFREQ = 8
NB = 1024


def set_ends(values, stream_key, least, top_value):
    longest = values.shape.index(max(values.shape))
    spots = []
    for shift in (0, 1):
        where = [jax.random.randint(jax.random.fold_in(stream_key, axis), (), 0, length) for axis, length in enumerate(values.shape)]
        where[longest] = (where[longest] + shift) % values.shape[longest]
        spots.append(tuple(where))
    return values.at[spots[0]].set(least).at[spots[1]].set(top_value)


def level_of(stream_key, extent, cuts, least, top_value):
    level, own = 1.0, jax.random.fold_in(stream_key, 6)
    for axis_at, blocks in cuts:
        heights = jnp.exp(jax.random.uniform(jax.random.fold_in(own, axis_at), (blocks,), jnp.float32, least / len(cuts), top_value / len(cuts)))
        level = level * jnp.repeat(heights, extent[axis_at] // blocks).reshape([-1 if axis == axis_at else 1 for axis in range(len(extent))])
    return level


def centred(rng, dims, scale, reach, cuts=(), kind=jnp.bfloat16):
    gain = level_of(rng, dims, cuts, -0.22, 0.18) if cuts else 1.0
    entries = jax.random.normal(rng, dims, jnp.float32) * scale * gain
    return jnp.minimum(jnp.maximum(entries, -reach), reach).astype(kind)


def setup_inputs(seed: int = 0) -> dict:
    key_list = jax.random.split(jax.random.key(seed), 7)
    pair_elements = centred(key_list[0], (NG, NB * 2 * STATES), 1.0, 6.0, ((0, 8), (1, 64)))
    screening = centred(key_list[1], (NG, NG), NG ** -0.5, 0.09375, ((0, 8), (1, 64)))
    energies = jnp.clip(jax.random.uniform(key_list[2], (NB,), jnp.float32, 0.5, 3.0), 0.5, 3.0)
    frequencies = jnp.clip(jnp.exp(jax.random.uniform(key_list[3], (NFREQ,), jnp.float32, math.log(0.3), math.log(3.0))), 0.3, 3.0)
    qp_index = set_ends(jax.random.randint(key_list[4], (STATES,), 0, NB), jax.random.fold_in(key_list[4], 1), 0, NB - 1).astype(jnp.int32)
    occupied = set_ends((jax.random.randint(key_list[5], (NB,), 0, 2) < 1).astype(jnp.int32), jax.random.fold_in(key_list[5], 1), 0, 1)
    return {"pair_elements": pair_elements, "screening": screening, "energies": energies, "frequencies": frequencies, "qp_index": qp_index, "occupied": occupied}


def band_weights(energies, frequencies, qp_index, occupied, offset, band_count):
    level_count = energies.shape[0]
    position = jnp.arange(level_count, dtype=jnp.int32)
    signed = jnp.where(occupied == 1, -energies, energies)
    onehot = (qp_index[:, None] == position[None, :]).astype(jnp.float32)
    state_level = jnp.sum(onehot * signed[None, :], axis=1)
    band_level = lax.dynamic_slice_in_dim(signed, offset, band_count, 0)
    detuning = state_level[:, None] - band_level[None, :]
    imag_freq = frequencies[:, None, None]
    modulus = detuning[None] ** 2 + imag_freq ** 2
    return detuning[None] / modulus, -imag_freq / modulus


def window_sigma(elements, screened, weight_real, weight_imag, band_count):
    row_count = elements.shape[0]
    local_elems = elements.astype(jnp.float32).reshape(row_count, band_count, 2, STATES)
    image_cols = screened.reshape(row_count, band_count, 2, STATES)
    intersection = jnp.einsum("gnpi,gnqj->npiqj", local_elems, image_cols, precision=lax.Precision.HIGHEST)
    intersection_real = intersection[:, 0, :, 0, :] + intersection[:, 1, :, 1, :]
    intersection_imag = intersection[:, 0, :, 1, :] - intersection[:, 1, :, 0, :]
    sigma_real = jnp.einsum("kin,nij->kij", weight_real, intersection_real, precision=lax.Precision.HIGHEST) - jnp.einsum("kin,nij->kij", weight_imag, intersection_imag, precision=lax.Precision.HIGHEST)
    sigma_imag = jnp.einsum("kin,nij->kij", weight_real, intersection_imag, precision=lax.Precision.HIGHEST) + jnp.einsum("kin,nij->kij", weight_imag, intersection_real, precision=lax.Precision.HIGHEST)
    return jnp.stack([sigma_real, sigma_imag]) / NG


def reference(pair_elements, screening, energies, frequencies, qp_index, occupied):
    window_count = energies.shape[0] // BAND_DEV
    col_count = BAND_DEV * 2 * STATES

    def band_window(window_index):
        column_start = (window_index * col_count).astype(jnp.int32)
        elements = lax.dynamic_slice_in_dim(pair_elements, column_start, col_count, 1)
        screened = jnp.dot(screening, elements, preferred_element_type=jnp.float32)
        band_start = (window_index * BAND_DEV).astype(jnp.int32)
        weight_real, weight_imag = band_weights(energies, frequencies, qp_index, occupied, band_start, BAND_DEV)
        return window_sigma(elements, screened, weight_real, weight_imag, BAND_DEV)

    windows = lax.map(band_window, jnp.arange(window_count, dtype=jnp.int32))
    return jnp.sum(windows, axis=0)
```

```python
import functools

import jax
import jax.numpy as jnp
from jax import lax
from jax.experimental import pallas as pl
from jax.experimental.pallas import tpu as pltpu
from jax.sharding import Mesh
from jax.sharding import PartitionSpec as P

STATES = 32
NG = 4096
NX, NY, NH = 4, 8, 4
ROWS = 512
COLS = 1024
BANDS = 16
BLK = ("y", "x", "zl")
GA = ("zh", "core")
MESH = pl.DeviceIdType.MESH
BF16, F32 = jnp.bfloat16, jnp.float32
PIECES = 4
PROWS = ROWS // PIECES


def kernel(
    m_ref, wt_ref, energy, freq, qp, occ, out_ref,
    mbuf, wown, wraw, slab, mt0, mt1, t1, t2, weight, sig, part, gath1, gath2, gath3, final,
    m_local, w_local, m_send, m_recv, f_send, f_recv, w_send, w_recv,
    ax_s, ax_r, ay_s, ay_r, by_s, by_r, bx_s, bx_r, r_send, r_recv,
):
    y, x = lax.axis_index("y"), lax.axis_index("x")
    zl, zh, k = lax.axis_index("zl"), lax.axis_index("zh"), lax.axis_index("core")
    other = 1 - k

    def up(v, d, n):
        return lax.rem(v + (d + n), n)

    def local(src, dst, sem):
        return pltpu.make_async_copy(src, dst, sem)

    def remote(src, dst, send, recv, **where):
        return pltpu.make_async_remote_copy(
            src_ref=src, dst_ref=dst, send_sem=send, recv_sem=recv,
            device_id=where, device_id_type=MESH,
        )

    own_m = local(m_ref, mbuf.at[0, k], m_local)
    own_m.start()
    own_w = local(wt_ref, wown, w_local.at[0])
    own_w.start()

    barrier = pltpu.get_barrier_semaphore()
    peers = []
    for step in range(1, 8):
        peers.append({"x": lax.rem(x + step // 2, NX), "core": lax.rem(k + step % 2, 2)})
        peers.append({"y": lax.rem(y + step, NY)})
        peers.append({"zh": lax.rem(zh + step // 2, NH), "zl": lax.rem(zl + step % 2, 2)})
    down_y, down_h = up(y, -2, NY), up(zh, -1, NH)
    over_y, over_h = up(y, 2, NY), up(zh, 1, NH)
    for side in range(2):
        peers.append({"y": down_y, "zh": down_h, "zl": jnp.int32(side)})
        peers.append({"y": over_y, "zh": over_h, "zl": jnp.int32(side)})
    for peer in peers:
        pl.semaphore_signal(barrier, inc=1, device_id=peer, device_id_type=MESH)

    def level(at):
        return jnp.where(occ[at] == 1, -energy[at], energy[at])

    sub = lax.broadcasted_iota(jnp.int32, (STATES, 128), 0)
    lane_freq = lax.broadcasted_iota(jnp.int32, (STATES, 128), 1) // STATES
    state = jnp.zeros((STATES, 128), F32)
    for i in range(STATES):
        state = jnp.where(sub == i, level(qp[i]), state)
    window = []
    for half in range(2):
        row = jnp.zeros((STATES, 128), F32)
        for j in range(4):
            row = jnp.where(lane_freq == j, freq[4 * half + j], row)
        window.append(row)
    band0 = ((y * NX + x) * 2 + zl) * BANDS

    @pl.loop(0, BANDS)
    def _(n):
        gap = state - level(band0 + n)
        for half in range(2):
            modulus = gap * gap + window[half] * window[half]
            weight[n, half, 0] = gap / modulus
            weight[n, half, 1] = -window[half] / modulus

    own_w.wait()
    pl.semaphore_wait(barrier, len(peers))

    special = (y // 2) == lax.rem(zh + 2, NH)

    @pl.when(jnp.logical_not(special))
    def _():
        remote(wown, wraw.at[zl], w_send.at[0], w_recv.at[zl], zl=1 - zl).start()
        local(wt_ref, wraw.at[zl], w_local.at[1]).start()

    @pl.when(special)
    def _():
        for side in range(2):
            remote(
                wown, wraw.at[zl], w_send.at[side], w_recv.at[zl],
                y=down_y, zh=down_h, zl=jnp.int32(side),
            ).start()

    own_m.wait()

    def m_rows(p):
        return pl.ds(p * PROWS, PROWS)

    def m_copy(p, way):
        src = mbuf.at[0, k, m_rows(p)]
        if way == 0:
            return remote(
                src, mbuf.at[2, k, m_rows(p)], m_send.at[0, p], m_recv.at[0, p], zh=up(zh, 1, NH)
            )
        if way == 1:
            return remote(
                src, mbuf.at[1, k, m_rows(p)], m_send.at[1, p], m_recv.at[1, p], zh=up(zh, -1, NH)
            )
        return remote(
            src, mbuf.at[0, k, m_rows(p)], m_send.at[2, p], m_recv.at[2, p], core=other
        )

    for p in range(PIECES):
        for way in range(2):
            m_copy(p, way).start()
    for p in range(PIECES):
        m_copy(p, 2).start()

    def m_landed(p, way):
        m_copy(p, way).wait_recv()

    def forward(p, way):
        place = mbuf.at[2 - way, k, m_rows(p)]
        return remote(place, place, f_send.at[way, p], f_recv.at[way, p], core=other)

    def pass_on(p):
        for way in range(2):
            m_landed(p, way)
            forward(p, way).start()

    @pl.when(jnp.logical_not(special))
    def _():
        remote(wown, wraw.at[1 - zl], w_send.at[0], w_recv.at[1 - zl], zl=1 - zl).wait_recv()
        local(wt_ref, wraw.at[zl], w_local.at[1]).wait()

    @pl.when(special)
    def _():
        for side in range(2):
            remote(
                wown, wraw.at[side], w_send.at[side], w_recv.at[side],
                y=down_y, zh=down_h, zl=jnp.int32(side),
            ).wait_recv()

    slab[y, x] = jnp.concatenate([wraw[0], wraw[1]], axis=0).T

    sign = (1, -1)

    def quarter(kind, h):
        return pl.ds((2 * kind + h) * 128, 128)

    def ax(h, i):
        s = sign[h]
        src = x if i < 2 else up(x, -s, NX)
        place = slab.at[y, src, quarter(0, h)]
        return remote(place, place, ax_s.at[h, i], ax_r.at[h, i], x=up(x, -s if i == 1 else s, NX))

    def ring_y(h, i):
        s = sign[h]
        if i < 4:
            return up(y, -s * i, NY), up(y, s, NY)
        return up(y, s * (i - 4), NY), up(y, -s, NY)

    def ay(h, i):
        src, to = ring_y(h, i)
        place = slab.at[src, :, quarter(0, h)]
        return remote(place, place, ay_s.at[h, i], ay_r.at[h, i], y=to)

    def by(h, i):
        src, to = ring_y(h, i)
        place = slab.at[src, x, quarter(1, h)]
        return remote(place, place, by_s.at[h, i], by_r.at[h, i], y=to)

    def bx(h, i):
        s = sign[h]
        src = x if i < 2 else up(x, -s, NX)
        place = slab.at[:, src, quarter(1, h)]
        return remote(place, place, bx_s.at[h, i], bx_r.at[h, i], x=up(x, -s if i == 1 else s, NX))

    def go(copy, *at):
        for h in range(2):
            for i in at:
                copy(h, i).start()

    def step(copy, *pairs):
        for h in range(2):
            for got, then in pairs:
                copy(h, got).wait_recv()
                if then is not None:
                    copy(h, then).start()

    go(by, 0, 4)
    go(ax, 0, 1)
    mt0[...] = mbuf[0, k].T
    step(ax, (0, 2))
    step(by, (0, 1), (4, 5))
    step(ax, (1, None), (2, None))
    go(ay, 0, 4)
    step(by, (1, 2), (5, 6))
    step(by, (2, 3), (6, None))
    step(ay, (0, 1), (4, 5))
    step(by, (3, None))
    go(bx, 0, 1)
    pass_on(0)
    step(ay, (1, 2), (5, 6))
    step(bx, (0, 2))
    pass_on(1)
    step(ay, (2, 3), (6, None))
    step(bx, (1, None), (2, None))
    step(ay, (3, None))
    pass_on(2)
    for p in range(PIECES):
        m_landed(p, 2)
    for p in range(PIECES - 1):
        for way in range(2):
            forward(p, way).wait_recv()

    chunk_of = (zh, up(zh, 1, NH), up(zh, -1, NH), up(zh, 2, NH))

    def w_block(chunk, p):
        base = 2 * chunk_of[chunk]
        return [slab[base, p], slab[base + 1, p]]

    def m_block(j, p, columns):
        return [mbuf[j, 0, m_rows(p), columns], mbuf[j, 1, m_rows(p), columns]]

    def multiply(terms, columns):
        left, right = [], []
        for chunk, j, p in terms:
            left += w_block(chunk, p)
            right += m_block(j, p, columns)
        return jnp.dot(
            jnp.concatenate(left, axis=1), jnp.concatenate(right, axis=0),
            preferred_element_type=F32,
        )

    early = [p for p in range(PIECES - 1)]
    last = PIECES - 1

    for p in early:
        mt1[:, pl.ds(p * PROWS, PROWS)] = mbuf[1, k, m_rows(p)].T

    @pl.loop(0, 4)
    def _(g):
        columns = pl.ds(pl.multiple_of(g * 256, 256), 256)
        own = [(0, 0, p) for p in range(PIECES)]
        t1[:, columns] = multiply(
            own + [(1, 1, p) for p in early] + [(2, 2, p) for p in early], columns
        )
        t2[:, columns] = multiply([(3, 2, p) for p in early], columns)

    pass_on(last)
    mt1[:, pl.ds(last * PROWS, PROWS)] = mbuf[1, k, m_rows(last)].T
    for way in range(2):
        forward(last, way).wait_recv()

    def split(value):
        high = value.astype(BF16)
        return [high, (value - high.astype(F32)).astype(BF16)]

    sig[...] = jnp.zeros_like(sig)

    @pl.loop(0, 4)
    def _(g):
        columns = pl.ds(pl.multiple_of(g * 256, 256), 256)
        first = t1[:, columns] + multiply([(1, 1, last), (2, 2, last)], columns)
        second = t2[:, columns] + multiply([(3, 2, last)], columns)
        left0, left1 = mt0[columns, :], mt1[columns, :]
        part[...] = jnp.dot(
            jnp.concatenate([left0, left0, left1, left1], axis=1),
            jnp.concatenate(split(first) + split(second), axis=0),
            preferred_element_type=F32,
        )
        sums = [sig[pl.ds(STATES * v, STATES), :] for v in range(4)]
        for b in range(4):
            block = part[pl.ds(64 * b, 64), :][:, 64 * b : 64 * b + 64]
            real = block[:STATES, :STATES] + block[STATES:, STATES:]
            imag = block[:STATES, STATES:] - block[STATES:, :STATES]
            real = jnp.concatenate([real] * 4, axis=1)
            imag = jnp.concatenate([imag] * 4, axis=1)
            for half in range(2):
                w_real = weight[4 * g + b, half, 0]
                w_imag = weight[4 * g + b, half, 1]
                sums[half] += w_real * real - w_imag * imag
                sums[2 + half] += w_real * imag + w_imag * real
        for v in range(4):
            sig[pl.ds(STATES * v, STATES), :] = sums[v]

    slot = 2 * x + k

    def every(phase, buffer):
        block = buffer.at[pl.ds(0, 7)]
        local(block, block, r_recv.at[phase]).wait()

    def drained(phase, buffer):
        block = buffer.at[pl.ds(0, 7)]
        local(block, block, r_send.at[phase]).wait()

    def total(buffer):
        value = buffer[0]
        for i in range(1, 8):
            value = value + buffer[i]
        return value

    def rows_of(i):
        return pl.ds(pl.multiple_of(i * 16, 16), 16)

    for hop in range(1, 8):
        to_x, to_k = lax.rem(x + hop // 2, NX), lax.rem(k + hop % 2, 2)
        remote(
            sig.at[rows_of(2 * to_x + to_k)], gath1.at[slot], r_send.at[0], r_recv.at[0],
            x=to_x, core=to_k,
        ).start()
    gath1[slot] = sig[rows_of(slot), :]
    every(0, gath1)
    gath2[y] = total(gath1)
    for hop in range(1, 8):
        remote(
            gath2.at[y], gath2.at[y], r_send.at[1], r_recv.at[1], y=lax.rem(y + hop, NY)
        ).start()
    every(1, gath2)
    place = 2 * zh + zl
    gath3[place] = total(gath2)
    for hop in range(1, 8):
        remote(
            gath3.at[place], gath3.at[place], r_send.at[2], r_recv.at[2],
            zh=lax.rem(zh + hop // 2, NH), zl=lax.rem(zl + hop % 2, 2),
        ).start()
    every(2, gath3)
    final[slot] = total(gath3) * (1.0 / NG)
    for hop in range(1, 8):
        remote(
            final.at[slot], final.at[slot], r_send.at[3], r_recv.at[3],
            x=lax.rem(x + hop // 2, NX), core=lax.rem(k + hop % 2, 2),
        ).start()
    every(3, final)
    for i in range(8):
        out_ref[pl.ds(16 * i, 16), :] = final[i]

    for p in range(PIECES):
        for way in range(3):
            m_copy(p, way).wait_send()
        for way in range(2):
            forward(p, way).wait_send()
    for h in range(2):
        for i in range(3):
            ax(h, i).wait_send()
            bx(h, i).wait_send()
        for i in range(7):
            ay(h, i).wait_send()
            by(h, i).wait_send()
    remote(wown, wraw.at[zl], w_send.at[0], w_recv.at[zl], zl=1 - zl).wait_send()

    @pl.when(special)
    def _():
        remote(wown, wraw.at[zl], w_send.at[1], w_recv.at[zl], zl=1 - zl).wait_send()

    drained(0, gath1)
    drained(1, gath2)
    drained(2, gath3)
    drained(3, final)


def shards(pair_elements, screening, energies, frequencies, qp_index, occupied):
    vmem = functools.partial(pltpu.VMEM)
    dma = pltpu.SemaphoreType.DMA
    smem = pl.BlockSpec(memory_space=pltpu.SMEM)
    anywhere = pl.BlockSpec(memory_space=pl.ANY)
    packed = pl.pallas_call(
        kernel,
        out_shape=jax.ShapeDtypeStruct((128, 128), F32),
        in_specs=[anywhere, anywhere, smem, smem, smem, smem],
        out_specs=pl.BlockSpec(memory_space=pltpu.VMEM),
        scratch_shapes=[
            vmem((3, 2, ROWS, COLS), BF16),
            vmem((64, ROWS), BF16),
            vmem((2, 64, ROWS), BF16),
            vmem((NY, NX, ROWS, 128), BF16),
            vmem((COLS, ROWS), BF16),
            vmem((COLS, ROWS), BF16),
            vmem((ROWS, COLS), F32),
            vmem((ROWS, COLS), F32),
            vmem((BANDS, 2, 2, STATES, 128), F32),
            vmem((128, 128), F32),
            vmem((256, 256), F32),
            vmem((8, 16, 128), F32),
            vmem((8, 16, 128), F32),
            vmem((8, 16, 128), F32),
            vmem((8, 16, 128), F32),
            dma,
            dma((2,)),
            dma((3, PIECES)),
            dma((3, PIECES)),
            dma((2, PIECES)),
            dma((2, PIECES)),
            dma((2,)),
            dma((2,)),
            dma((2, 3)),
            dma((2, 3)),
            dma((2, 7)),
            dma((2, 7)),
            dma((2, 7)),
            dma((2, 7)),
            dma((2, 3)),
            dma((2, 3)),
            dma((4,)),
            dma((4,)),
        ],
        compiler_params=pltpu.CompilerParams(collective_id=0, has_side_effects=True),
    )(pair_elements, screening.T, energies, frequencies, qp_index, occupied)
    packed = packed.reshape(2, 2, STATES, 4, STATES)
    return packed.transpose(0, 1, 3, 2, 4).reshape(2, 8, STATES, STATES)


def solution(mesh):
    torus = Mesh(mesh.devices.reshape(NY, NX, 2, NH, 2), ("y", "x", "zl", "zh", "core"))
    in_specs = (P(GA, BLK), P(GA, BLK), P(), P(), P(), P())
    return jax.shard_map(
        shards, mesh=torus, in_specs=in_specs, out_specs=P(), check_vma=False
    )
```

```python
import functools

import jax
import jax.numpy as jnp
from jax import lax
from jax.experimental import pallas as pl
from jax.experimental.pallas import tpu as pltpu
from jax.sharding import Mesh
from jax.sharding import PartitionSpec as P

STATES = 32
NG = 4096
NX, NY, NH = 4, 8, 4
ROWS = 512
COLS = 1024
BANDS = 16
BLK = ("y", "x", "zl")
GA = ("zh", "core")
MESH = pl.DeviceIdType.MESH
BF16, F32 = jnp.bfloat16, jnp.float32
PIECES = 4
PROWS = ROWS // PIECES


def kernel(
    m_ref, wt_ref, energy, freq, qp, occ, out_ref,
    mbuf, wown, wraw, slab, mt0, mt1, t1, t2, weight, sig, part, gath1, gath2, gath3, final,
    m_local, w_local, m_send, m_recv, f_send, f_recv, w_send, w_recv,
    ax_s, ax_r, ay_s, ay_r, by_s, by_r, bx_s, bx_r, r_send, r_recv,
):
    y, x = lax.axis_index("y"), lax.axis_index("x")
    zl, zh, k = lax.axis_index("zl"), lax.axis_index("zh"), lax.axis_index("core")
    other = 1 - k

    def up(v, d, n):
        return lax.rem(v + (d + n), n)

    def local(src, dst, sem):
        return pltpu.make_async_copy(src, dst, sem)

    def remote(src, dst, send, recv, **where):
        return pltpu.make_async_remote_copy(
            src_ref=src, dst_ref=dst, send_sem=send, recv_sem=recv,
            device_id=where, device_id_type=MESH,
        )

    own_m = local(m_ref, mbuf.at[0, k], m_local)
    own_m.start()
    own_w = local(wt_ref, wown, w_local.at[0])
    own_w.start()

    barrier = pltpu.get_barrier_semaphore()
    peers = []
    for step in range(1, 8):
        peers.append({"x": lax.rem(x + step // 2, NX), "core": lax.rem(k + step % 2, 2)})
        peers.append({"y": lax.rem(y + step, NY)})
        peers.append({"zh": lax.rem(zh + step // 2, NH), "zl": lax.rem(zl + step % 2, 2)})
    down_y, down_h = up(y, -2, NY), up(zh, -1, NH)
    over_y, over_h = up(y, 2, NY), up(zh, 1, NH)
    for side in range(2):
        peers.append({"y": down_y, "zh": down_h, "zl": jnp.int32(side)})
        peers.append({"y": over_y, "zh": over_h, "zl": jnp.int32(side)})
    for peer in peers:
        pl.semaphore_signal(barrier, inc=1, device_id=peer, device_id_type=MESH)

    def level(at):
        return jnp.where(occ[at] == 1, -energy[at], energy[at])

    sub = lax.broadcasted_iota(jnp.int32, (STATES, 128), 0)
    lane_freq = lax.broadcasted_iota(jnp.int32, (STATES, 128), 1) // STATES
    state = jnp.zeros((STATES, 128), F32)
    for i in range(STATES):
        state = jnp.where(sub == i, level(qp[i]), state)
    window = []
    for half in range(2):
        row = jnp.zeros((STATES, 128), F32)
        for j in range(4):
            row = jnp.where(lane_freq == j, freq[4 * half + j], row)
        window.append(row)
    band0 = ((y * NX + x) * 2 + zl) * BANDS

    @pl.loop(0, BANDS)
    def _(n):
        gap = state - level(band0 + n)
        for half in range(2):
            modulus = gap * gap + window[half] * window[half]
            weight[n, half, 0] = gap / modulus
            weight[n, half, 1] = -window[half] / modulus

    own_w.wait()
    pl.semaphore_wait(barrier, len(peers))

    special = (y // 2) == lax.rem(zh + 2, NH)

    @pl.when(jnp.logical_not(special))
    def _():
        remote(wown, wraw.at[zl], w_send.at[0], w_recv.at[zl], zl=1 - zl).start()
        local(wt_ref, wraw.at[zl], w_local.at[1]).start()

    @pl.when(special)
    def _():
        for side in range(2):
            remote(
                wown, wraw.at[zl], w_send.at[side], w_recv.at[zl],
                y=down_y, zh=down_h, zl=jnp.int32(side),
            ).start()

    def m_rows(p):
        return pl.ds(p * PROWS, PROWS)

    def m_copy(p, way):
        src = mbuf.at[0, k, m_rows(p)]
        if way == 0:
            return remote(
                src, mbuf.at[2, k, m_rows(p)], m_send.at[0, p], m_recv.at[0, p], zh=up(zh, 1, NH)
            )
        if way == 1:
            return remote(
                src, mbuf.at[1, k, m_rows(p)], m_send.at[1, p], m_recv.at[1, p], zh=up(zh, -1, NH)
            )
        return remote(
            src, mbuf.at[0, k, m_rows(p)], m_send.at[2, p], m_recv.at[2, p], core=other
        )

    def m_landed(p, way):
        m_copy(p, way).wait_recv()

    def forward(p, way):
        place = mbuf.at[2 - way, k, m_rows(p)]
        return remote(place, place, f_send.at[way, p], f_recv.at[way, p], core=other)

    def pass_on(p):
        for way in range(2):
            m_landed(p, way)
            forward(p, way).start()

    @pl.when(jnp.logical_not(special))
    def _():
        remote(wown, wraw.at[1 - zl], w_send.at[0], w_recv.at[1 - zl], zl=1 - zl).wait_recv()
        local(wt_ref, wraw.at[zl], w_local.at[1]).wait()

    @pl.when(special)
    def _():
        for side in range(2):
            remote(
                wown, wraw.at[side], w_send.at[side], w_recv.at[side],
                y=down_y, zh=down_h, zl=jnp.int32(side),
            ).wait_recv()

    own_m.wait()
    for p in range(PIECES):
        for way in range(2):
            m_copy(p, way).start()
    slab[y, x] = jnp.concatenate([wraw[0], wraw[1]], axis=0).T

    sign = (1, -1)

    def quarter(kind, h):
        return pl.ds((2 * kind + h) * 128, 128)

    def ax(h, i):
        s = sign[h]
        src = x if i < 2 else up(x, -s, NX)
        place = slab.at[y, src, quarter(0, h)]
        return remote(place, place, ax_s.at[h, i], ax_r.at[h, i], x=up(x, -s if i == 1 else s, NX))

    def ring_y(h, i):
        s = sign[h]
        if i < 4:
            return up(y, -s * i, NY), up(y, s, NY)
        return up(y, s * (i - 4), NY), up(y, -s, NY)

    def ay(h, i):
        src, to = ring_y(h, i)
        place = slab.at[src, :, quarter(0, h)]
        return remote(place, place, ay_s.at[h, i], ay_r.at[h, i], y=to)

    def by(h, i):
        src, to = ring_y(h, i)
        place = slab.at[src, x, quarter(1, h)]
        return remote(place, place, by_s.at[h, i], by_r.at[h, i], y=to)

    def bx(h, i):
        s = sign[h]
        src = x if i < 2 else up(x, -s, NX)
        place = slab.at[:, src, quarter(1, h)]
        return remote(place, place, bx_s.at[h, i], bx_r.at[h, i], x=up(x, -s if i == 1 else s, NX))

    def go(copy, *at):
        for h in range(2):
            for i in at:
                copy(h, i).start()

    def step(copy, *pairs):
        for h in range(2):
            for got, then in pairs:
                copy(h, got).wait_recv()
                if then is not None:
                    copy(h, then).start()

    go(by, 0, 4)
    go(ax, 0, 1)
    for p in range(PIECES):
        m_copy(p, 2).start()
    mt0[...] = mbuf[0, k].T
    step(ax, (0, 2))
    step(by, (0, 1), (4, 5))
    step(ax, (1, None), (2, None))
    go(ay, 0, 4)
    step(by, (1, 2), (5, 6))
    step(by, (2, 3), (6, None))
    step(ay, (0, 1), (4, 5))
    step(by, (3, None))
    go(bx, 0, 1)
    step(ay, (1, 2), (5, 6))
    step(bx, (0, 2))
    step(ay, (2, 3), (6, None))
    step(bx, (1, None), (2, None))
    step(ay, (3, None))
    for p in range(PIECES):
        m_landed(p, 2)
    for p in range(PIECES - 1):
        pass_on(p)
    for p in range(PIECES - 1):
        for way in range(2):
            forward(p, way).wait_recv()

    chunk_of = (zh, up(zh, 1, NH), up(zh, -1, NH), up(zh, 2, NH))

    def w_block(chunk, p):
        base = 2 * chunk_of[chunk]
        return [slab[base, p], slab[base + 1, p]]

    def m_block(j, p, columns):
        return [mbuf[j, 0, m_rows(p), columns], mbuf[j, 1, m_rows(p), columns]]

    def multiply(terms, columns):
        left, right = [], []
        for chunk, j, p in terms:
            left += w_block(chunk, p)
            right += m_block(j, p, columns)
        return jnp.dot(
            jnp.concatenate(left, axis=1), jnp.concatenate(right, axis=0),
            preferred_element_type=F32,
        )

    early = [p for p in range(PIECES - 1)]
    last = PIECES - 1

    for p in early:
        mt1[:, pl.ds(p * PROWS, PROWS)] = mbuf[1, k, m_rows(p)].T

    @pl.loop(0, 4)
    def _(g):
        columns = pl.ds(pl.multiple_of(g * 256, 256), 256)
        own = [(0, 0, p) for p in range(PIECES)]
        t1[:, columns] = multiply(
            own + [(1, 1, p) for p in early] + [(2, 2, p) for p in early], columns
        )
        t2[:, columns] = multiply([(3, 2, p) for p in early], columns)

    pass_on(last)
    mt1[:, pl.ds(last * PROWS, PROWS)] = mbuf[1, k, m_rows(last)].T
    for way in range(2):
        forward(last, way).wait_recv()

    def split(value):
        high = value.astype(BF16)
        return [high, (value - high.astype(F32)).astype(BF16)]

    sig[...] = jnp.zeros_like(sig)

    @pl.loop(0, 4)
    def _(g):
        columns = pl.ds(pl.multiple_of(g * 256, 256), 256)
        first = t1[:, columns] + multiply([(1, 1, last), (2, 2, last)], columns)
        second = t2[:, columns] + multiply([(3, 2, last)], columns)
        left0, left1 = mt0[columns, :], mt1[columns, :]
        part[...] = jnp.dot(
            jnp.concatenate([left0, left0, left1, left1], axis=1),
            jnp.concatenate(split(first) + split(second), axis=0),
            preferred_element_type=F32,
        )
        sums = [sig[pl.ds(STATES * v, STATES), :] for v in range(4)]
        for b in range(4):
            block = part[pl.ds(64 * b, 64), :][:, 64 * b : 64 * b + 64]
            real = block[:STATES, :STATES] + block[STATES:, STATES:]
            imag = block[:STATES, STATES:] - block[STATES:, :STATES]
            real = jnp.concatenate([real] * 4, axis=1)
            imag = jnp.concatenate([imag] * 4, axis=1)
            for half in range(2):
                w_real = weight[4 * g + b, half, 0]
                w_imag = weight[4 * g + b, half, 1]
                sums[half] += w_real * real - w_imag * imag
                sums[2 + half] += w_real * imag + w_imag * real
        for v in range(4):
            sig[pl.ds(STATES * v, STATES), :] = sums[v]

    slot = 2 * x + k

    def every(phase, buffer):
        block = buffer.at[pl.ds(0, 7)]
        local(block, block, r_recv.at[phase]).wait()

    def drained(phase, buffer):
        block = buffer.at[pl.ds(0, 7)]
        local(block, block, r_send.at[phase]).wait()

    def total(buffer):
        value = buffer[0]
        for i in range(1, 8):
            value = value + buffer[i]
        return value

    def rows_of(i):
        return pl.ds(pl.multiple_of(i * 16, 16), 16)

    for hop in range(1, 8):
        to_x, to_k = lax.rem(x + hop // 2, NX), lax.rem(k + hop % 2, 2)
        remote(
            sig.at[rows_of(2 * to_x + to_k)], gath1.at[slot], r_send.at[0], r_recv.at[0],
            x=to_x, core=to_k,
        ).start()
    gath1[slot] = sig[rows_of(slot), :]
    every(0, gath1)
    place = 2 * zh + zl
    chip = total(gath1)
    gath2[0, y] = chip[:8]
    gath2[1, place] = chip[8:]

    def to_y(hop):
        return {"y": lax.rem(y + hop, NY)}

    def to_z(hop):
        return {"zh": lax.rem(zh + hop // 2, NH), "zl": lax.rem(zl + hop % 2, 2)}

    def spread(buffer, phase, way, at, to):
        for hop in range(1, 8):
            remote(
                buffer.at[way, at], buffer.at[way, at], r_send.at[phase], r_recv.at[phase],
                **to(hop),
            ).start()

    spread(gath2, 1, 0, y, to_y)
    spread(gath2, 2, 1, place, to_z)
    every(1, gath2.at[0])
    gath3[0, place] = total(gath2.at[0])
    spread(gath3, 3, 0, place, to_z)
    every(2, gath2.at[1])
    gath3[1, y] = total(gath2.at[1])
    spread(gath3, 4, 1, y, to_y)
    every(3, gath3.at[0])
    every(4, gath3.at[1])
    final[slot] = jnp.concatenate(
        [total(gath3.at[0]), total(gath3.at[1])], axis=0
    ) * (1.0 / NG)
    for hop in range(1, 8):
        remote(
            final.at[slot], final.at[slot], r_send.at[5], r_recv.at[5],
            x=lax.rem(x + hop // 2, NX), core=lax.rem(k + hop % 2, 2),
        ).start()
    every(5, final)
    for v in range(4):
        block = jnp.concatenate([final[2 * v], final[2 * v + 1]], axis=0)
        for j in range(4):
            out_ref[v // 2, 4 * (v % 2) + j] = block[:, STATES * j : STATES * (j + 1)]

    for p in range(PIECES):
        for way in range(3):
            m_copy(p, way).wait_send()
        for way in range(2):
            forward(p, way).wait_send()
    for h in range(2):
        for i in range(3):
            ax(h, i).wait_send()
            bx(h, i).wait_send()
        for i in range(7):
            ay(h, i).wait_send()
            by(h, i).wait_send()
    remote(wown, wraw.at[zl], w_send.at[0], w_recv.at[zl], zl=1 - zl).wait_send()

    @pl.when(special)
    def _():
        remote(wown, wraw.at[zl], w_send.at[1], w_recv.at[zl], zl=1 - zl).wait_send()

    drained(0, gath1)
    drained(1, gath2.at[0])
    drained(2, gath2.at[1])
    drained(3, gath3.at[0])
    drained(4, gath3.at[1])
    drained(5, final)


def shards(pair_elements, screening, energies, frequencies, qp_index, occupied):
    vmem = functools.partial(pltpu.VMEM)
    dma = pltpu.SemaphoreType.DMA
    smem = pl.BlockSpec(memory_space=pltpu.SMEM)
    anywhere = pl.BlockSpec(memory_space=pl.ANY)
    return pl.pallas_call(
        kernel,
        out_shape=jax.ShapeDtypeStruct((2, 8, STATES, STATES), F32),
        in_specs=[anywhere, anywhere, smem, smem, smem, smem],
        out_specs=pl.BlockSpec(memory_space=pltpu.VMEM),
        scratch_shapes=[
            vmem((3, 2, ROWS, COLS), BF16),
            vmem((64, ROWS), BF16),
            vmem((2, 64, ROWS), BF16),
            vmem((NY, NX, ROWS, 128), BF16),
            vmem((COLS, ROWS), BF16),
            vmem((COLS, ROWS), BF16),
            vmem((ROWS, COLS), F32),
            vmem((ROWS, COLS), F32),
            vmem((BANDS, 2, 2, STATES, 128), F32),
            vmem((128, 128), F32),
            vmem((256, 256), F32),
            vmem((8, 16, 128), F32),
            vmem((2, 8, 8, 128), F32),
            vmem((2, 8, 8, 128), F32),
            vmem((8, 16, 128), F32),
            dma,
            dma((2,)),
            dma((3, PIECES)),
            dma((3, PIECES)),
            dma((2, PIECES)),
            dma((2, PIECES)),
            dma((2,)),
            dma((2,)),
            dma((2, 3)),
            dma((2, 3)),
            dma((2, 7)),
            dma((2, 7)),
            dma((2, 7)),
            dma((2, 7)),
            dma((2, 3)),
            dma((2, 3)),
            dma((6,)),
            dma((6,)),
        ],
        compiler_params=pltpu.CompilerParams(collective_id=0, has_side_effects=True),
    )(pair_elements, screening.T, energies, frequencies, qp_index, occupied)


def solution(mesh):
    torus = Mesh(mesh.devices.reshape(NY, NX, 2, NH, 2), ("y", "x", "zl", "zh", "core"))
    in_specs = (P(GA, BLK), P(GA, BLK), P(), P(), P(), P())
    return jax.shard_map(
        shards, mesh=torus, in_specs=in_specs, out_specs=P(), check_vma=False
    )
```
